32 devices in a mesh: layer: 4 (over y, x), energy: 8 (over z, core).
Axes of the slice: x: 2, y: 2, z: 4, core: 2. Of those that a mesh axis runs over, the one named last changes fastest.
Arguments:
- onsite: float32 [4, 256], P('layer'), may hold values from -1 to 1
- broadening: float32 [4, 256], P('layer'), may hold values from 1 to 2
- hamiltonian: float32 [4, 2, 256, 256], P('layer'), may hold values from -0.078125 to 0.078125
- coupling: float32 [4, 2, 256, 256], P('layer'), may hold values from -0.21875 to 0.21875
- coupling_mask: int32 [4, 256, 256], P('layer'), may hold values 0 or 1
- prior_sigma: float32 [4, 32, 2, 256, 256], P('layer', 'energy'), may hold values from -0.4 to 0.4, as said below
- kernel_weights: float32 [8], replicated, may hold values from 0.1 to 0.6
- kernel_offsets: int32 [8], replicated, may hold values from -7 to 7
Outputs:
- self_energy: float32 [4, 32, 2, 256, 256], P('layer', 'energy')
The draws below stay inside these ranges and needn't reach their ends.
Inputs may be any that keep to these rules, and one draw needn't show every extreme that they name: `prior_sigma`: real and imaginary parts of the blocks.
All inputs are finite; a program needn't handle non-finite values. No bound on the sum of `coupling_mask` on one device may be relied on, other than what follows from the above.
Results may differ from the reference program's by a relative error of at most 0.0001.
Values sent between devices are 32-bit elements; how exact they have to be, the bound alone decides.
No kernel may reach another device: no remote copies, remote signals or barrier semaphores. Data moves between devices by JAX's collectives and lax.ppermute only.
A program may use at most 128 MiB of HBM per device.

```python
import math
import jax
import jax.numpy as jnp
from jax import lax

M = 256
NS_ITERS = 3
TAPS = 8
ENERGIES = 32
REACH = 7
N_LAYER = 4


def draw_prior_sigma(key, part):
    key_off, key_diag = jax.random.split(jax.random.fold_in(key, 11))
    full_shape = (N_LAYER, ENERGIES, 2, M, M)
    diag_shape = (N_LAYER, ENERGIES, 2, M)
    spread = jax.random.truncated_normal(key_off, -4.0, 4.0, full_shape, jnp.float32) * (0.1 / math.sqrt(M))
    local = jax.random.truncated_normal(key_diag, -4.0, 4.0, diag_shape, jnp.float32) * 0.1
    identity = jnp.eye(M, dtype=jnp.float32)
    return spread * (1.0 - identity) + local[..., None] * identity


def place_ends(result, stream_key, least, largest):
    longest = result.shape.index(max(result.shape))
    spots = []
    for shift in (0, 1):
        where = [jax.random.randint(jax.random.fold_in(stream_key, axis), (), 0, length) for axis, length in enumerate(result.shape)]
        where[longest] = (where[longest] + shift) % result.shape[longest]
        spots.append(tuple(where))
    return result.at[spots[0]].set(least).at[spots[1]].set(largest)


def level_of(rng, extent, cuts, low, high):
    gain = 1.0
    for axis_at, shards_of in cuts:
        heights = jax.random.uniform(jax.random.fold_in(jax.random.fold_in(rng, 6), axis_at), (shards_of,), jnp.float32, low / len(cuts), high / len(cuts))
        gain = gain * jnp.repeat(jnp.exp(heights), extent[axis_at] // shards_of).reshape((-1,) + (1,) * (len(extent) - 1 - axis_at))
    return gain


def scatter_about(own_key, dims, scale, limit, pieces=(), kind=jnp.bfloat16):
    drawn = jax.random.normal(own_key, dims, jnp.float32) * scale
    if len(pieces) > 0:
        drawn = level_of(own_key, dims, pieces, -0.22, 0.18) * drawn
    return jnp.clip(drawn, min=-limit, max=limit).astype(kind)


def setup_inputs(seed: int = 0) -> dict:
    arg_keys = jax.random.split(jax.random.key(seed), 9)
    onsite = jnp.clip(jax.random.uniform(arg_keys[0], (N_LAYER, M), jnp.float32, -1.0, 1.0) * level_of(arg_keys[0], (N_LAYER, M), ((0, 4),), -0.4, 0.0), -1.0, 1.0)
    broadening = jnp.clip(jnp.exp(math.log(2.0) - 0.6931472 * jax.random.uniform(arg_keys[1], (N_LAYER, M), jnp.float32) ** level_of(arg_keys[1], (N_LAYER, M), ((0, 4),), -0.2, 0.2)), 1.0, 2.0)
    hamiltonian = scatter_about(arg_keys[2], (N_LAYER, 2, M, M), (25 * M) ** -0.5, 0.078125, ((0, 4),), jnp.float32)
    coupling = scatter_about(arg_keys[3], (N_LAYER, 2, M, M), (3 * M) ** -0.5, 0.21875, ((0, 4),), jnp.float32)
    coupling_mask = place_ends((jax.random.randint(arg_keys[4], (N_LAYER, M, M), 0, 2) < 1).astype(jnp.int32), jax.random.fold_in(arg_keys[4], 1), 0, 1)
    prior_sigma = draw_prior_sigma(jax.random.fold_in(arg_keys[8], 71), 0)
    kernel_weights = jnp.clip(jax.random.uniform(arg_keys[6], (TAPS,), jnp.float32, 0.1, 0.6), 0.1, 0.6)
    kernel_offsets = place_ends(jax.random.randint(arg_keys[7], (TAPS,), 0 - REACH, REACH + 1), jax.random.fold_in(arg_keys[7], 1), 0 - REACH, REACH).astype(jnp.int32)
    return dict(onsite=onsite, broadening=broadening, hamiltonian=hamiltonian, coupling=coupling, coupling_mask=coupling_mask, prior_sigma=prior_sigma, kernel_weights=kernel_weights, kernel_offsets=kernel_offsets)


exact_mode = lax.Precision.HIGHEST


def matmul_high(first_op, second_op):
    return jnp.matmul(first_op, second_op, precision=exact_mode)


def complex_product(first_op, second_op):
    first_real = first_op[..., 0, :, :]
    first_imag = first_op[..., 1, :, :]
    second_real = second_op[..., 0, :, :]
    second_imag = second_op[..., 1, :, :]
    real_part = matmul_high(first_real, second_real) - matmul_high(first_imag, second_imag)
    imag_part = matmul_high(first_real, second_imag) + matmul_high(first_imag, second_real)
    return jnp.stack([real_part, imag_part], axis=-3)


def adjoint(matrix):
    return jnp.stack([jnp.swapaxes(matrix[..., 0, :, :], -1, -2), -jnp.swapaxes(matrix[..., 1, :, :], -1, -2)], axis=-3)


def lead_block(batch_size, orbitals):
    identity = jnp.eye(orbitals, dtype=jnp.float32)
    single = jnp.stack([jnp.zeros_like(identity), -0.5 * identity])
    return jnp.broadcast_to(single, (batch_size, 2, orbitals, orbitals))


def energy_levels(positions, grid_size):
    return -1.0 + 2.0 * (positions.astype(jnp.float32) + 0.5) / grid_size


def solve_layer(levels, onsite_row, damping_row, hamilton, coupler, pattern, previous, incoming, sweeps):
    orbitals = hamilton.shape[-1]
    identity = jnp.eye(orbitals, dtype=jnp.float32)
    hermitian = 0.5 * (hamilton + adjoint(hamilton))
    masked = coupler * pattern.astype(jnp.float32)[None]
    contact = complex_product(complex_product(masked[None], incoming), adjoint(masked)[None])
    real_diag = levels[:, None] - onsite_row[None, :]
    imag_diag = jnp.broadcast_to(damping_row[None, :], real_diag.shape)
    shifted = jnp.stack([real_diag, imag_diag], axis=1)[..., None, :] * identity
    system = shifted - hermitian[None] - contact - previous
    diag_real = jnp.diagonal(system[:, 0], axis1=-2, axis2=-1)
    diag_imag = jnp.diagonal(system[:, 1], axis1=-2, axis2=-1)
    modulus = diag_real * diag_real + diag_imag * diag_imag
    inverse = jnp.stack([diag_real / modulus, -diag_imag / modulus], axis=1)[..., None, :] * identity
    for sweep_no in range(sweeps):
        residue = complex_product(system, inverse)
        inverse = 2.0 * inverse - complex_product(inverse, residue)
    return inverse


def convolution_matrix(weights, offsets, row_count, col_count, margin):
    row_idx = jnp.arange(row_count, dtype=jnp.int32)
    col_idx = jnp.arange(col_count, dtype=jnp.int32)
    matches = col_idx[None, None, :] == row_idx[None, :, None] + margin + offsets[:, None, None]
    return jnp.sum(jnp.where(matches, weights[:, None, None], jnp.float32(0.0)), axis=0)


def reference(onsite, broadening, hamiltonian, coupling, coupling_mask, prior_sigma, kernel_weights, kernel_offsets):
    levels = energy_levels(jnp.arange(ENERGIES, dtype=jnp.int32), ENERGIES)
    incoming = lead_block(ENERGIES, M)
    green_list = []
    for layer_no in range(N_LAYER):
        incoming = solve_layer(levels, onsite[layer_no], broadening[layer_no], hamiltonian[layer_no], coupling[layer_no], coupling_mask[layer_no], prior_sigma[layer_no], incoming, NS_ITERS)
        green_list.append(incoming)
    kernel = convolution_matrix(kernel_weights, kernel_offsets, ENERGIES, ENERGIES, 0)
    outputs = [jnp.einsum("fe,epij->fpij", kernel, green_block, precision=exact_mode) for green_block in green_list]
    return jnp.stack(outputs)
```

```python
import functools

import jax
import jax.numpy as jnp
from jax import lax
from jax.experimental import pallas as pl
from jax.experimental.pallas import tpu as pltpu
from jax.sharding import PartitionSpec as P

NS_ITERS = 3
REACH = 7

AXES = ("layer", "energy")
F32 = jnp.float32
BF16 = jnp.bfloat16
HBM = pltpu.HBM
VMEM = pltpu.VMEM


def split(x):
    high = x.astype(BF16)
    low = (x - high.astype(F32)).astype(BF16)
    return high, low


def dot(a, b, transposed):
    dims = (((1,), (1 if transposed else 0,)), ((), ()))
    return lax.dot_general(a, b, dims, preferred_element_type=F32)


def dot3(a, b, transposed=False):
    return (
        dot(a[0], b[0], transposed) + dot(a[0], b[1], transposed) + dot(a[1], b[0], transposed)
    )


def negated(a):
    return (-a[0], -a[1])


def product(a, b):
    real = dot3(a[0], b[0]) + dot3(negated(a[1]), b[1])
    imag = dot3(a[0], b[1]) + dot3(a[1], b[0])
    return real, imag


def product_adjoint(a, c):
    real = dot3(a[0], c[0], True) + dot3(a[1], c[1], True)
    imag = dot3(a[1], c[0], True) + dot3(negated(a[0]), c[1], True)
    return real, imag


def split_pair(pair):
    return split(pair[0]), split(pair[1])


def eye_mask(n):
    return lax.broadcasted_iota(jnp.int32, (n, n), 0) == lax.broadcasted_iota(
        jnp.int32, (n, n), 1
    )


def inverse_of(real, imag):
    n = real.shape[0]
    eye = eye_mask(n)
    zero = jnp.zeros_like(real)
    diag_real = jnp.where(eye, real, zero)
    diag_imag = jnp.where(eye, imag, zero)

    def reciprocal(axis):
        dr = jnp.sum(diag_real, axis=axis, keepdims=True)
        di = jnp.sum(diag_imag, axis=axis, keepdims=True)
        modulus = dr * dr + di * di
        return dr / modulus, -di / modulus

    row_r, row_i = reciprocal(0)
    col_r, col_i = reciprocal(1)
    e_r = jnp.where(eye, zero, real * -row_r + imag * row_i)
    e_i = jnp.where(eye, zero, real * -row_i - imag * row_r)
    unit = jnp.where(eye, 1.0, 0.0).astype(F32)
    f_r, f_i = unit + e_r, e_i
    for _ in range(NS_ITERS - 1):
        es = split_pair((e_r, e_i))
        e_r, e_i = product(es, es)
        es = split_pair((e_r, e_i))
        g_r, g_i = product(split_pair((f_r, f_i)), es)
        f_r, f_i = f_r + g_r, f_i + g_i
    return col_r * f_r - col_i * f_i, col_r * f_i + col_i * f_r


def prep_kernel(
    where_ref, levels_ref, onsite_ref, broad_ref, ham_ref, coup_ref, mask_ref, prior_ref,
    *out_refs
):
    layer_count = prior_ref.shape[1]
    base_refs = out_refs[:layer_count]
    masked_ref, send_ref = out_refs[layer_count:]
    layer, core = where_ref[0], where_ref[1]
    n = ham_ref.shape[-1]
    mask = mask_ref[0].astype(F32)
    c_r, c_i = coup_ref[0, 0] * mask, coup_ref[0, 1] * mask
    masked_ref[0], masked_ref[1] = c_r, c_i
    send_ref[...] = masked_ref[core]
    h_r, h_i = ham_ref[0, 0], ham_ref[0, 1]
    eye = eye_mask(n)
    cs = split_pair((c_r, c_i))
    q_r, q_i = product_adjoint(cs, cs)
    first = jnp.where(layer == 0, 0.5, 0.0).astype(F32)
    fixed_r = -0.5 * (h_r + h_r.T) - first * q_i + jnp.where(eye, -onsite_ref[...], 0.0)
    fixed_i = -0.5 * (h_i - h_i.T) + first * q_r + jnp.where(eye, broad_ref[...], 0.0)
    for k in range(layer_count):
        mine = jnp.bitwise_xor(layer, k)
        level = levels_ref[mine]
        base_refs[k][0] = fixed_r - prior_ref[0, mine, 0] + jnp.where(eye, level, 0.0)
        base_refs[k][1] = fixed_i - prior_ref[0, mine, 1]


def first_kernel(where_ref, *refs):
    layer_count = len(refs) - 3
    base_refs, green_ref, base, sem = refs[:layer_count], refs[-3], refs[-2], refs[-1]
    mine = where_ref[0]
    for k in range(layer_count):
        @pl.when(mine == k)
        def _(k=k):
            copy = pltpu.make_async_copy(base_refs[k], base, sem)
            copy.start()
            copy.wait()
    green_ref[0], green_ref[1] = inverse_of(base[0], base[1])


def rest_kernel(layer_count, where_ref, *refs):
    refs = list(refs)
    take = lambda count: [refs.pop(0) for _ in range(count)]
    base_refs = take(layer_count)
    (masked_ref,) = take(1)
    same_refs, other_refs = take(layer_count - 1), take(layer_count - 1)
    (green_in,) = take(1)
    out_refs = take(layer_count)
    bases, coups, greens, in_sems, out_sems = refs
    layer, core = where_ref[0], where_ref[1]
    other = 1 - core

    def inputs(l, k):
        if k == 0:
            pairs = [(masked_ref, coups.at[l])]
        else:
            pairs = [
                (same_refs[k - 1], coups.at[l, core]),
                (other_refs[k - 1], coups.at[l, other]),
            ]
        pairs.append((base_refs[k], bases.at[l]))
        return [pltpu.make_async_copy(s, d, in_sems.at[l, i]) for i, (s, d) in enumerate(pairs)]

    for l in range(1, layer_count):
        for k in range(layer_count):
            @pl.when(jnp.bitwise_xor(layer, l) == k)
            def _(l=l, k=k):
                for copy in inputs(l, k):
                    copy.start()
    greens[0] = green_in[...]

    def output(l, k):
        return pltpu.make_async_copy(greens.at[l], out_refs[k], out_sems.at[k])

    def put(l):
        for k in range(layer_count):
            @pl.when(jnp.bitwise_xor(layer, l) == k)
            def _(k=k):
                output(l, k).start()

    put(0)
    for l in range(1, layer_count):
        for k in range(layer_count):
            @pl.when(jnp.bitwise_xor(layer, l) == k)
            def _(l=l, k=k):
                for copy in inputs(l, k):
                    copy.wait()

    def step(l, carry):
        cs = split_pair((coups[l, 0], coups[l, 1]))
        moved = product(cs, split_pair((greens[l - 1, 0], greens[l - 1, 1])))
        contact_r, contact_i = product_adjoint(split_pair(moved), cs)
        greens[l, 0], greens[l, 1] = inverse_of(
            bases[l, 0] - contact_r, bases[l, 1] - contact_i
        )
        put(l)
        return carry

    lax.fori_loop(1, layer_count, step, 0)
    for k in range(layer_count):
        output(0, k).wait()


def mix_kernel(has_acc, weight_ref, *refs):
    refs = list(refs)
    out_ref = refs.pop()
    acc_ref = refs.pop(0) if has_acc else None
    outputs, _, rows, _ = out_ref.shape[1:]
    step_rows = 8

    def body(i, carry):
        part = i // (rows // step_rows)
        here = pl.ds(pl.multiple_of((i % (rows // step_rows)) * step_rows, step_rows), step_rows)
        if has_acc:
            total = [acc_ref[0, f, part, here, :] for f in range(outputs)]
        else:
            total = [None] * outputs
        for j, ref in enumerate(refs):
            x = ref[part, here, :]
            for f in range(outputs):
                term = weight_ref[f, j] * x
                total[f] = term if total[f] is None else total[f] + term
        for f in range(outputs):
            out_ref[0, f, part, here, :] = total[f]
        return carry

    lax.fori_loop(0, 2 * (rows // step_rows), body, 0)


def mix(weights, acc, blocks, outputs):
    _, n, _ = blocks[0].shape
    rows = 64 if n % 64 == 0 else n
    small = pl.BlockSpec((2, rows, n), lambda i: (0, i, 0))
    large = pl.BlockSpec((1, outputs, 2, rows, n), lambda i: (0, 0, 0, i, 0))
    head = [] if acc is None else [acc]
    return pl.pallas_call(
        functools.partial(mix_kernel, acc is not None),
        grid=(n // rows,),
        in_specs=[pl.BlockSpec(memory_space=pltpu.SMEM)]
        + [large] * len(head)
        + [small] * len(blocks),
        out_specs=large,
        out_shape=jax.ShapeDtypeStruct((1, outputs, 2, n, n), F32),
        name="mix_more" if head else "mix_first",
    )(weights, *head, *blocks)


def weights_for(kernel_weights, kernel_offsets, rows, columns):
    matches = columns[None, None, :] == rows[None, :, None] + kernel_offsets[:, None, None]
    return jnp.sum(jnp.where(matches, kernel_weights[:, None, None], F32(0.0)), axis=0)


def local(
    onsite, broadening, hamiltonian, coupling, coupling_mask, prior_sigma,
    kernel_weights, kernel_offsets,
):
    layer_count = lax.axis_size("layer")
    group_count = lax.axis_size("energy")
    per_device = prior_sigma.shape[1]
    n = prior_sigma.shape[-1]
    grid_size = per_device * group_count
    span = 2 * per_device
    assert per_device == layer_count and layer_count & (layer_count - 1) == 0
    assert group_count % 2 == 0 and span > REACH
    layer = lax.axis_index("layer")
    group = lax.axis_index("energy")
    core, pair = group % 2, group // 2
    where = jnp.stack([layer, core]).astype(jnp.int32)
    block = jax.ShapeDtypeStruct((2, n, n), F32)
    smem = pl.BlockSpec(memory_space=pltpu.SMEM)
    hbm = pl.BlockSpec(memory_space=HBM)
    vmem = pl.BlockSpec(memory_space=VMEM)

    everyone = [(l, g) for l in range(layer_count) for g in range(group_count)]

    def move(x, target, wanted=lambda l, g: True):
        pairs = []
        for l, g in everyone:
            if not wanted(l, g):
                continue
            tl, tg = target(l, g)
            if 0 <= tg < group_count:
                pairs.append((l * group_count + g, tl * group_count + tg))
        return lax.ppermute(x, AXES, pairs)

    def to_layer(x, k):
        return move(x, lambda l, g: (l ^ k, g))

    own = group * per_device + jnp.arange(per_device, dtype=jnp.int32)
    levels = -1.0 + 2.0 * (own.astype(F32) + 0.5) / grid_size
    prepared = pl.pallas_call(
        prep_kernel,
        in_specs=[smem, smem] + [vmem] * 6,
        out_specs=[vmem] * (layer_count + 2),
        out_shape=[block] * (layer_count + 1) + [jax.ShapeDtypeStruct((n, n), F32)],
        name="prep",
    )(where, levels, onsite, broadening, hamiltonian, coupling, coupling_mask, prior_sigma)
    bases, masked, half = list(prepared[:layer_count]), prepared[-2], prepared[-1]
    ks = range(1, layer_count)
    bases = bases[:1] + [to_layer(bases[k], k) for k in ks]
    same = [to_layer(half, k) for k in ks]
    other = [move(x, lambda l, g: (l, g ^ 1)) for x in same]
    green = pl.pallas_call(
        first_kernel,
        in_specs=[smem] + [hbm] * layer_count,
        out_specs=vmem,
        out_shape=block,
        scratch_shapes=[VMEM((2, n, n), F32), pltpu.SemaphoreType.DMA],
        name="solve_first",
    )(where, *bases)
    greens = pl.pallas_call(
        functools.partial(rest_kernel, layer_count),
        in_specs=[smem] + [hbm] * (layer_count + 1 + 2 * len(ks)) + [vmem],
        out_specs=[hbm] * layer_count,
        out_shape=[block] * layer_count,
        scratch_shapes=[
            VMEM((layer_count, 2, n, n), F32),
            VMEM((layer_count, 2, n, n), F32),
            VMEM((layer_count, 2, n, n), F32),
            pltpu.SemaphoreType.DMA((layer_count, 3)),
            pltpu.SemaphoreType.DMA((layer_count,)),
        ],
        name="solve_rest",
    )(where, *bases, masked, *same, *other, green)

    mine = [greens[0]] + [to_layer(greens[k], k) for k in ks]

    def energy_in_pair(l, g, k):
        return per_device * (g % 2) + (l ^ k)

    up, down, theirs, cross = [], [], [], []
    for k in range(layer_count):
        up.append(
            move(
                mine[k],
                lambda l, g: (l, g + 2),
                lambda l, g: span - energy_in_pair(l, g, k) <= REACH,
            )
        )
        down.append(
            move(
                mine[k],
                lambda l, g: (l, g - 2),
                lambda l, g: energy_in_pair(l, g, k) + 1 <= REACH,
            )
        )
        theirs.append(move(mine[k], lambda l, g: (l, g ^ 1)))
        cross.append(
            (
                move(up[k], lambda l, g: (l, g - 1), lambda l, g: g % 2 == 1),
                move(down[k], lambda l, g: (l, g + 1), lambda l, g: g % 2 == 0),
            )
        )

    def energy(shift, c, k):
        return span * (pair + shift) + per_device * c + jnp.bitwise_xor(layer, k)

    def mixed(acc, entries):
        columns = jnp.stack([e for _, e in entries])
        w = weights_for(kernel_weights, kernel_offsets, own, columns)
        return mix(w, acc, [x for x, _ in entries], per_device)

    def far(k):
        return [
            (up[k], energy(-1, core, k)),
            (down[k], energy(1, core, k)),
            (cross[k][0], energy(-1, 1 - core, k)),
            (cross[k][1], energy(1, 1 - core, k)),
        ]

    near = []
    for k in range(layer_count):
        near += [(mine[k], energy(0, core, k)), (theirs[k], energy(0, 1 - core, k))]
    acc = mixed(None, near)
    acc = mixed(acc, [entry for k in range(layer_count - 1) for entry in far(k)])
    return mixed(acc, far(layer_count - 1))


def solution(mesh):
    placed = (
        P("layer", None),
        P("layer", None),
        P("layer", None, None, None),
        P("layer", None, None, None),
        P("layer", None, None),
        P("layer", "energy", None, None, None),
        P(),
        P(),
    )
    return jax.shard_map(
        local,
        mesh=mesh,
        in_specs=placed,
        out_specs=P("layer", "energy", None, None, None),
        check_vma=False,
    )
```

```python
import functools

import jax
import jax.numpy as jnp
from jax import lax
from jax.experimental import pallas as pl
from jax.experimental.pallas import tpu as pltpu
from jax.sharding import PartitionSpec as P


NS_ITERS = 3
REACH = 7

AXES = ("layer", "energy")
F32 = jnp.float32
BF16 = jnp.bfloat16
HBM = pltpu.HBM
VMEM = pltpu.VMEM


def split(x):
    high = x.astype(BF16)
    low = (x - high.astype(F32)).astype(BF16)
    return high, low


def dot(a, b, transposed):
    dims = (((1,), (1 if transposed else 0,)), ((), ()))
    return lax.dot_general(a, b, dims, preferred_element_type=F32)


def dot3(a, b, transposed=False):
    return (
        dot(a[0], b[0], transposed) + dot(a[0], b[1], transposed) + dot(a[1], b[0], transposed)
    )


def negated(a):
    return (-a[0], -a[1])


def product(a, b):
    real = dot3(a[0], b[0]) + dot3(negated(a[1]), b[1])
    imag = dot3(a[0], b[1]) + dot3(a[1], b[0])
    return real, imag


def product_adjoint(a, c):
    real = dot3(a[0], c[0], True) + dot3(a[1], c[1], True)
    imag = dot3(a[1], c[0], True) + dot3(negated(a[0]), c[1], True)
    return real, imag


def split_pair(pair):
    return split(pair[0]), split(pair[1])


def eye_mask(n):
    return lax.broadcasted_iota(jnp.int32, (n, n), 0) == lax.broadcasted_iota(
        jnp.int32, (n, n), 1
    )


def inverse_of(real, imag):
    n = real.shape[0]
    eye = eye_mask(n)
    zero = jnp.zeros_like(real)
    diag_real = jnp.where(eye, real, zero)
    diag_imag = jnp.where(eye, imag, zero)

    def reciprocal(axis):
        dr = jnp.sum(diag_real, axis=axis, keepdims=True)
        di = jnp.sum(diag_imag, axis=axis, keepdims=True)
        modulus = dr * dr + di * di
        return dr / modulus, -di / modulus

    row_r, row_i = reciprocal(0)
    col_r, col_i = reciprocal(1)
    e_r = jnp.where(eye, zero, real * -row_r + imag * row_i)
    e_i = jnp.where(eye, zero, real * -row_i - imag * row_r)
    unit = jnp.where(eye, 1.0, 0.0).astype(F32)
    f_r, f_i = unit + e_r, e_i
    for _ in range(NS_ITERS - 1):
        es = split_pair((e_r, e_i))
        e_r, e_i = product(es, es)
        es = split_pair((e_r, e_i))
        g_r, g_i = product(split_pair((f_r, f_i)), es)
        f_r, f_i = f_r + g_r, f_i + g_i
    return col_r * f_r - col_i * f_i, col_r * f_i + col_i * f_r


def prep_kernel(
    coup_hbm, mask_hbm, ham_hbm, onsite_hbm, broad_hbm, prior_hbm, masked_ref, quarter_ref, *refs
):
    base_refs = refs[:-7]
    coup_ref, mask_ref, ham_ref, onsite_ref, broad_ref, prior_ref, sems = refs[-7:]
    sources = (coup_hbm, mask_hbm, ham_hbm, onsite_hbm, broad_hbm, prior_hbm)
    targets = (coup_ref, mask_ref, ham_ref, onsite_ref, broad_ref, prior_ref)
    copies = [
        pltpu.make_async_copy(source, target, sems.at[i])
        for i, (source, target) in enumerate(zip(sources, targets))
    ]
    for copy in copies:
        copy.start()
    per_device = prior_ref.shape[1]
    layer = lax.axis_index("layer")
    group = lax.axis_index("energy")
    plane, half = group % 2, (group // 2) % 2
    rows = quarter_ref.shape[0]
    for copy in copies[:2]:
        copy.wait()
    mask = mask_ref[0].astype(F32)
    c_r, c_i = coup_ref[0, 0] * mask, coup_ref[0, 1] * mask
    masked_ref[0], masked_ref[1] = c_r, c_i
    here = pl.ds(pl.multiple_of(half * rows, rows), rows)
    quarter_ref[...] = masked_ref[plane, here, :]
    cs = split_pair((c_r, c_i))
    q_r, q_i = product_adjoint(cs, cs)
    for copy in copies[2:5]:
        copy.wait()
    first = group * per_device
    grid_size = per_device * lax.axis_size("energy")
    n = ham_ref.shape[-1]
    h_r, h_i = ham_ref[0, 0], ham_ref[0, 1]
    eye = eye_mask(n)
    own = jnp.where(layer == 0, 0.5, 0.0).astype(F32)
    fixed_r = -0.5 * (h_r + h_r.T) - own * q_i + jnp.where(eye, -onsite_ref[...], 0.0)
    fixed_i = -0.5 * (h_i - h_i.T) + own * q_r + jnp.where(eye, broad_ref[...], 0.0)
    copies[5].wait()
    for k, base_ref in enumerate(base_refs):
        mine = jnp.bitwise_xor(layer, k)
        level = -1.0 + 2.0 * ((first + mine).astype(F32) + 0.5) / grid_size
        base_ref[0] = fixed_r - prior_ref[0, mine, 0] + jnp.where(eye, level, 0.0)
        base_ref[1] = fixed_i - prior_ref[0, mine, 1]


def stack_kernel(*refs):
    out_ref = refs[-1]
    for k, ref in enumerate(refs[:-1]):
        out_ref[k] = ref[...]


def join_kernel(near_ref, far_ref, out_ref):
    half = (lax.axis_index("energy") // 2) % 2
    rows = near_ref.shape[1]
    for side, ref in ((half, near_ref), (1 - half, far_ref)):
        out_ref[:, pl.ds(pl.multiple_of(side * rows, rows), rows), :] = ref[...]


def solve_kernel(layer_count, *refs):
    base_refs = refs[:layer_count]
    masked_ref, same_ref, other_ref = refs[layer_count : layer_count + 3]
    out_refs = refs[layer_count + 3 : 2 * layer_count + 3]
    system, coup, green = refs[2 * layer_count + 3 :]
    layer = lax.axis_index("layer")
    core = lax.axis_index("energy") % 2

    def step(l, carry):
        source = jnp.bitwise_xor(layer, l)
        for k in range(layer_count):
            @pl.when(source == k)
            def _(k=k):
                system[...] = base_refs[k][...]
                if k == 0:
                    coup[...] = masked_ref[...]
                else:
                    coup[core] = same_ref[k - 1]
                    coup[1 - core] = other_ref[k - 1]

        @pl.when(l > 0)
        def _():
            cs = split_pair((coup[0], coup[1]))
            moved = product(cs, split_pair((green[0], green[1])))
            contact_r, contact_i = product_adjoint(split_pair(moved), cs)
            system[0] -= contact_r
            system[1] -= contact_i

        g_r, g_i = inverse_of(system[0], system[1])
        green[0], green[1] = g_r, g_i
        for k in range(layer_count):
            @pl.when(source == k)
            def _(k=k):
                out_refs[k][0], out_refs[k][1] = g_r, g_i
        return carry

    lax.fori_loop(0, layer_count, step, 0)


STEP_ROWS = 16


def weight_kernel(value_ref, offset_ref, out_ref):
    layer = lax.axis_index("layer")
    group = lax.axis_index("energy")
    layer_count = lax.axis_size("layer")
    per_device = layer_count
    span = 2 * per_device
    core = group % 2
    shape = out_ref.shape
    row = lax.broadcasted_iota(jnp.int32, shape, 0)
    lane = lax.broadcasted_iota(jnp.int32, shape, 1)
    kind = lane // layer_count
    away = 2 * core - 1
    shift = jnp.where(kind == INNER, -away, jnp.where(kind == CROSSED, away, 0))
    shift = jnp.where(kind == OUTER, away, shift)
    far_core = jnp.where((kind == THEIRS) | (kind == CROSSED), 1 - core, core)
    source = jnp.bitwise_xor(lane % layer_count, layer)
    gap = span * shift + per_device * far_core + source - (per_device * core + row)
    total = jnp.zeros(shape, F32)
    for tap in range(value_ref.shape[0]):
        total += jnp.where(gap == offset_ref[tap], value_ref[tap], 0.0)
    out_ref[...] = total


MINE, THEIRS, INNER, CROSSED, OUTER = range(5)


def mix_rows(weight_ref, slots, acc, refs, outputs, part, start):
    here = pl.ds(pl.multiple_of(start, STEP_ROWS), STEP_ROWS)
    total = [None] * outputs if acc is None else [acc[0, f, part, here, :] for f in range(outputs)]
    for slot, ref in zip(slots, refs):
        x = ref[part, here, :]
        for f in range(outputs):
            term = weight_ref[f, slot] * x
            total[f] = term if total[f] is None else total[f] + term
    return here, total


def mix_kernel(slots, has_acc, weight_ref, *refs):
    refs = list(refs)
    out_ref = refs.pop()
    acc_ref = refs.pop(0) if has_acc else None
    outputs, parts, rows, _ = out_ref.shape[1:]
    for part in range(parts):
        def body(i, carry, part=part):
            here, total = mix_rows(
                weight_ref, slots, acc_ref, refs, outputs, part, i * STEP_ROWS
            )
            for f in range(outputs):
                out_ref[0, f, part, here, :] = total[f]
            return carry

        lax.fori_loop(0, rows // STEP_ROWS, body, 0, unroll=2)


def last_kernel(slots, weight_ref, *refs):
    acc_ref, blocks, out_ref, buffer, sems = refs[0], refs[1:-3], refs[-3], refs[-2], refs[-1]
    outputs, parts, rows, _ = out_ref.shape[1:]
    pieces = 2
    size = rows // pieces
    copies = []
    for part in range(parts):
        for piece in range(pieces):
            def body(i, carry, part=part, base=piece * size):
                here, total = mix_rows(
                    weight_ref, slots, acc_ref, blocks, outputs, part, base + i * STEP_ROWS
                )
                for f in range(outputs):
                    buffer[0, f, part, here, :] = total[f]
                return carry

            lax.fori_loop(0, size // STEP_ROWS, body, 0, unroll=2)
            here = (slice(None), slice(None), part, pl.ds(piece * size, size))
            copy = pltpu.make_async_copy(buffer.at[here], out_ref.at[here], sems.at[part, piece])
            copy.start()
            copies.append(copy)
    for copy in copies:
        copy.wait()


SMEM_SPEC = pl.BlockSpec(memory_space=pltpu.SMEM)
VMEM_SPEC = pl.BlockSpec(memory_space=VMEM)
HBM_SPEC = pl.BlockSpec(memory_space=HBM)


def run(kernel, arrays, out_shape, head=(), scratch=(), space=VMEM, **more):
    arrays = [pltpu.with_memory_space_constraint(x, space) for x in arrays]
    return pl.pallas_call(
        kernel,
        in_specs=[SMEM_SPEC] * len(head) + [pl.BlockSpec(memory_space=space)] * len(arrays),
        out_shape=out_shape,
        scratch_shapes=list(scratch),
        compiler_params=pltpu.CompilerParams(vmem_limit_bytes=24 * 2**20),
        **({"out_specs": jax.tree.map(lambda _: VMEM_SPEC, out_shape)} | more),
    )(*head, *arrays)


def sweep(
    onsite, broadening, hamiltonian, coupling, coupling_mask, prior_sigma,
    kernel_weights, kernel_offsets,
):
    layer_count = lax.axis_size("layer")
    group_count = lax.axis_size("energy")
    per_device = prior_sigma.shape[1]
    n = prior_sigma.shape[-1]
    span = 2 * per_device
    assert per_device == layer_count and layer_count & (layer_count - 1) == 0
    assert group_count % 4 == 0 and span > REACH
    ks = range(1, layer_count)

    everyone = [(l, g) for l in range(layer_count) for g in range(group_count)]

    def move(x, target, wanted=lambda l, g: True):
        pairs = []
        for l, g in everyone:
            tl, tg = target(l, g)
            if wanted(l, g) and 0 <= tg < group_count:
                pairs.append((l * group_count + g, tl * group_count + tg))
        return lax.ppermute(x, AXES, pairs)

    def to_layer(x, k):
        return move(x, lambda l, g: (l ^ k, g))

    def swapped(x):
        return move(x, lambda l, g: (l, g ^ 1))

    block = VMEM((2, n, n), F32)
    inputs = [coupling, coupling_mask, hamiltonian, onsite, broadening, prior_sigma]
    masked, quarter, *bases = run(
        prep_kernel, inputs, [block, VMEM((n // 2, n), F32)] + [block] * layer_count,
        scratch=[VMEM(x.shape, x.dtype) for x in inputs]
        + [pltpu.SemaphoreType.DMA((len(inputs),))],
        space=HBM,
    )
    quarters = [to_layer(quarter, k) for k in ks]
    bases = [bases[0]] + [to_layer(bases[k], k) for k in ks]
    weights = run(
        weight_kernel, [], VMEM((8 * -(-per_device // 8), 128), F32),
        [kernel_weights, kernel_offsets],
    )
    near = run(stack_kernel, quarters, VMEM((len(ks), n // 2, n), F32))
    far = move(near, lambda l, g: (l, g ^ 2))
    same = run(join_kernel, [near, far], VMEM((len(ks), n, n), F32))
    other = swapped(same)
    greens = run(
        functools.partial(solve_kernel, layer_count),
        [*bases, masked, same, other], [block] * layer_count, scratch=[block] * 3,
    )

    mine = [greens[0]] + [to_layer(greens[k], k) for k in ks]

    def reached(l, g, k, step):
        spot = per_device * (g % 2) + (l ^ k)
        return (span - spot if step > 0 else spot + 1) <= REACH

    inner, outer, theirs, crossed = [], [], [], []
    for k in range(layer_count):
        def beyond(sign, k=k):
            step = lambda g: sign * (4 * (g % 2) - 2)
            return move(
                mine[k], lambda l, g: (l, g + step(g)),
                lambda l, g: reached(l, g, k, step(g)),
            )

        inner.append(beyond(1))
        outer.append(beyond(-1))
        theirs.append(swapped(mine[k]))
        crossed.append(swapped(inner[k]))

    shape = (1, per_device, 2, n, n)
    kinds = {MINE: mine, THEIRS: theirs, INNER: inner, CROSSED: crossed, OUTER: outer}

    def mixed(acc, entries, name):
        slots = tuple(kind * layer_count + k for kind, k in entries)
        blocks = [kinds[kind][k] for kind, k in entries]
        if name == "mix_last":
            return run(
                functools.partial(last_kernel, slots), [acc] + blocks,
                jax.ShapeDtypeStruct(shape, F32), [weights],
                [VMEM(shape, F32), pltpu.SemaphoreType.DMA((2, 2))], out_specs=HBM_SPEC,
            )
        kernel = functools.partial(mix_kernel, slots, acc is not None)
        return run(kernel, ([] if acc is None else [acc]) + blocks, VMEM(shape, F32), [weights])

    final = layer_count - 1
    acc = mixed(None, [(MINE, 0)], "mix_own")
    for k in ks[:-1]:
        acc = mixed(acc, [(MINE, k), (THEIRS, k - 1)], f"mix_next{k}")
    acc = mixed(acc, [(MINE, final), (THEIRS, final - 1), (THEIRS, final)], "mix_near")
    outside = (INNER, CROSSED, OUTER)
    acc = mixed(acc, [(kind, k) for kind in outside for k in range(final)], "mix_far")
    return mixed(acc, [(kind, final) for kind in outside], "mix_last")


def solution(mesh):
    placed = (
        P("layer", None),
        P("layer", None),
        P("layer", None, None, None),
        P("layer", None, None, None),
        P("layer", None, None),
        P("layer", "energy", None, None, None),
        P(),
        P(),
    )
    return jax.shard_map(
        sweep,
        mesh=mesh,
        in_specs=placed,
        out_specs=P("layer", "energy", None, None, None),
        check_vma=False,
    )
```

```python
import functools

import jax
import jax.numpy as jnp
from jax import lax
from jax.experimental import pallas as pl
from jax.experimental.pallas import tpu as pltpu
from jax.sharding import PartitionSpec as P


NS_ITERS = 3
REACH = 7

AXES = ("layer", "energy")
F32 = jnp.float32
BF16 = jnp.bfloat16
HBM = pltpu.HBM
VMEM = pltpu.VMEM


def split(x):
    high = x.astype(BF16)
    low = (x - high.astype(F32)).astype(BF16)
    return high, low


def dot(a, b, transposed):
    dims = (((1,), (1 if transposed else 0,)), ((), ()))
    return lax.dot_general(a, b, dims, preferred_element_type=F32)


def dot3(a, b, transposed=False):
    left = jnp.concatenate([a[0], a[0], a[1]], axis=1)
    right = jnp.concatenate([b[0], b[1], b[0]], axis=1 if transposed else 0)
    return dot(left, right, transposed)


def product(a, b):
    rr = dot3(a[0], b[0])
    ii = dot3(a[1], b[1])
    return rr - ii, dot3(a[2], b[2]) - rr - ii


def product_adjoint(a, c):
    rr = dot3(a[0], c[0], True)
    ii = dot3(a[1], c[1], True)
    return rr + ii, dot3(a[2], c[3], True) - rr + ii


def split_pair(pair):
    return split(pair[0]), split(pair[1]), split(pair[0] + pair[1]), split(pair[0] - pair[1])


def eye_mask(n):
    return lax.broadcasted_iota(jnp.int32, (n, n), 0) == lax.broadcasted_iota(
        jnp.int32, (n, n), 1
    )


def inverse_of(real, imag):
    n = real.shape[0]
    eye = eye_mask(n)
    zero = jnp.zeros_like(real)
    diag_real = jnp.where(eye, real, zero)
    diag_imag = jnp.where(eye, imag, zero)

    def reciprocal(axis):
        dr = jnp.sum(diag_real, axis=axis, keepdims=True)
        di = jnp.sum(diag_imag, axis=axis, keepdims=True)
        modulus = dr * dr + di * di
        return dr / modulus, -di / modulus

    row_r, row_i = reciprocal(0)
    col_r, col_i = reciprocal(1)
    e_r = jnp.where(eye, zero, real * -row_r + imag * row_i)
    e_i = jnp.where(eye, zero, real * -row_i - imag * row_r)
    unit = jnp.where(eye, 1.0, 0.0).astype(F32)
    f_r, f_i = unit + e_r, e_i
    for _ in range(NS_ITERS - 1):
        es = split_pair((e_r, e_i))
        e_r, e_i = product(es, es)
        es = split_pair((e_r, e_i))
        g_r, g_i = product(split_pair((f_r, f_i)), es)
        f_r, f_i = f_r + g_r, f_i + g_i
    return col_r * f_r - col_i * f_i, col_r * f_i + col_i * f_r


def prep_kernel(
    coup_hbm, mask_hbm, ham_hbm, onsite_hbm, broad_hbm, prior_hbm, masked_ref, quarter_ref, *refs
):
    base_refs = refs[:-7]
    coup_ref, mask_ref, ham_ref, onsite_ref, broad_ref, prior_ref, sems = refs[-7:]
    sources = (coup_hbm, mask_hbm, ham_hbm, onsite_hbm, broad_hbm, prior_hbm)
    targets = (coup_ref, mask_ref, ham_ref, onsite_ref, broad_ref, prior_ref)
    copies = [
        pltpu.make_async_copy(source, target, sems.at[i])
        for i, (source, target) in enumerate(zip(sources, targets))
    ]
    for copy in copies:
        copy.start()
    per_device = prior_ref.shape[1]
    layer = lax.axis_index("layer")
    group = lax.axis_index("energy")
    plane, half = group % 2, (group // 2) % 2
    rows = quarter_ref.shape[0]
    for copy in copies[:2]:
        copy.wait()
    mask = mask_ref[0].astype(F32)
    c_r, c_i = coup_ref[0, 0] * mask, coup_ref[0, 1] * mask
    masked_ref[0], masked_ref[1] = c_r, c_i
    here = pl.ds(pl.multiple_of(half * rows, rows), rows)
    quarter_ref[...] = masked_ref[plane, here, :]
    cs = split_pair((c_r, c_i))
    q_r, q_i = product_adjoint(cs, cs)
    for copy in copies[2:5]:
        copy.wait()
    first = group * per_device
    grid_size = per_device * lax.axis_size("energy")
    n = ham_ref.shape[-1]
    h_r, h_i = ham_ref[0, 0], ham_ref[0, 1]
    eye = eye_mask(n)
    own = jnp.where(layer == 0, 0.5, 0.0).astype(F32)
    fixed_r = -0.5 * (h_r + h_r.T) - own * q_i + jnp.where(eye, -onsite_ref[...], 0.0)
    fixed_i = -0.5 * (h_i - h_i.T) + own * q_r + jnp.where(eye, broad_ref[...], 0.0)
    copies[5].wait()
    for k, base_ref in enumerate(base_refs):
        mine = jnp.bitwise_xor(layer, k)
        level = -1.0 + 2.0 * ((first + mine).astype(F32) + 0.5) / grid_size
        base_ref[0] = fixed_r - prior_ref[0, mine, 0] + jnp.where(eye, level, 0.0)
        base_ref[1] = fixed_i - prior_ref[0, mine, 1]


def stack_kernel(*refs):
    out_ref = refs[-1]
    for k, ref in enumerate(refs[:-1]):
        out_ref[k] = ref[...]


def join_kernel(near_ref, far_ref, out_ref):
    half = (lax.axis_index("energy") // 2) % 2
    rows = near_ref.shape[1]
    for side, ref in ((half, near_ref), (1 - half, far_ref)):
        out_ref[:, pl.ds(pl.multiple_of(side * rows, rows), rows), :] = ref[...]


def solve_kernel(layer_count, *refs):
    refs = list(refs)
    take = lambda count: [refs.pop(0) for _ in range(count)]
    (own_base,) = take(1)
    base_refs = [take(layer_count - 1) for _ in range(2)]
    masked_ref, same_ref, other_ref = take(3)
    out_refs = take(layer_count)
    system, coup, green = refs
    layer = lax.axis_index("layer")
    core = lax.axis_index("energy") % 2

    def step(l, carry):
        source = jnp.bitwise_xor(layer, l)

        @pl.when(source == 0)
        def _():
            system[...] = own_base[...]
            coup[...] = masked_ref[...]

        for k in range(1, layer_count):
            @pl.when(source == k)
            def _(k=k):
                coup[core] = same_ref[k - 1]
                coup[1 - core] = other_ref[k - 1]

            for c in range(2):
                @pl.when((source == k) & (core == c))
                def _(k=k, c=c):
                    system[...] = base_refs[c][k - 1][...]

        @pl.when(l > 0)
        def _():
            cs = split_pair((coup[0], coup[1]))
            moved = product(cs, split_pair((green[0], green[1])))
            contact_r, contact_i = product_adjoint(split_pair(moved), cs)
            system[0] -= contact_r
            system[1] -= contact_i

        g_r, g_i = inverse_of(system[0], system[1])
        green[0], green[1] = g_r, g_i
        for k in range(layer_count):
            @pl.when(source == k)
            def _(k=k):
                out_refs[k][0], out_refs[k][1] = g_r, g_i
        return carry

    lax.fori_loop(0, layer_count, step, 0)


STEP_ROWS = 16


MINE, INNER, OUTER, CROSSED = range(4)


def weight_kernel(value_ref, offset_ref, out_ref):
    layer = lax.axis_index("layer")
    core = lax.axis_index("energy") % 2
    layer_count = lax.axis_size("layer")
    per_device = layer_count
    shape = out_ref.shape
    row = lax.broadcasted_iota(jnp.int32, shape, 0)
    lane = lax.broadcasted_iota(jnp.int32, shape, 1)
    kind = lane // layer_count
    away = 2 * core - 1
    shift = jnp.where(kind == INNER, -away, jnp.where(kind == MINE, 0, away))
    far_core = jnp.where(kind == CROSSED, 1 - core, core)
    source = jnp.bitwise_xor(lane % layer_count, layer)
    target = jnp.where(row < per_device, per_device * core, -per_device * core) + row
    gap = 2 * per_device * shift + per_device * far_core + source - target
    total = jnp.zeros(shape, F32)
    for tap in range(value_ref.shape[0]):
        total += jnp.where(gap == offset_ref[tap], value_ref[tap], 0.0)
    out_ref[...] = total


STEP_ROWS = 8


def add_blocks(total, weight_ref, slots, refs, part, here, first_row):
    total = list(total)
    for slot, ref in zip(slots, refs):
        x = ref[part, here, :]
        for f in range(len(total)):
            term = weight_ref[first_row + f, slot] * x
            total[f] = term if total[f] is None else total[f] + term
    return total


def tick_kernel(in_ref, out_ref):
    out_ref[...] = in_ref[...]


def mix_kernel(both, single, has_acc, weight_ref, *refs):
    refs = list(refs)
    own_ref, partner_ref = refs[-2:]
    accs = refs[:2] if has_acc else None
    blocks = refs[2 if has_acc else 0 : -2]
    outputs, parts, rows, _ = own_ref.shape
    for part in range(parts):
        def body(i, carry, part=part):
            here = pl.ds(pl.multiple_of(i * STEP_ROWS, STEP_ROWS), STEP_ROWS)
            for side, (target, slots) in enumerate(
                ((own_ref, both + single), (partner_ref, both))
            ):
                total = [accs[side][f, part, here, :] if has_acc else None for f in range(outputs)]
                total = add_blocks(
                    total, weight_ref, slots, blocks[: len(slots)], part, here, side * outputs
                )
                for f in range(outputs):
                    target[f, part, here, :] = total[f]
            return carry

        lax.fori_loop(0, rows // STEP_ROWS, body, 0, unroll=2)


def last_kernel(slots, weight_ref, own_ref, partner_ref, *refs):
    blocks, out_ref, buffer, sems = refs[:-3], refs[-3], refs[-2], refs[-1]
    outputs, parts, rows, _ = own_ref.shape
    pieces = sems.shape[1]
    size = rows // pieces
    copies = []
    for part in range(parts):
        for piece in range(pieces):
            def body(i, carry, part=part, base=piece * size):
                here = pl.ds(pl.multiple_of(base + i * STEP_ROWS, STEP_ROWS), STEP_ROWS)
                total = [
                    own_ref[f, part, here, :] + partner_ref[f, part, here, :]
                    for f in range(outputs)
                ]
                total = add_blocks(total, weight_ref, slots, blocks, part, here, 0)
                for f in range(outputs):
                    buffer[0, f, part, here, :] = total[f]
                return carry

            lax.fori_loop(0, size // STEP_ROWS, body, 0, unroll=4)
            here = (slice(None), slice(None), part, pl.ds(piece * size, size))
            copy = pltpu.make_async_copy(buffer.at[here], out_ref.at[here], sems.at[part, piece])
            copy.start()
            copies.append(copy)
    for copy in copies:
        copy.wait()


SMEM_SPEC = pl.BlockSpec(memory_space=pltpu.SMEM)
VMEM_SPEC = pl.BlockSpec(memory_space=VMEM)
HBM_SPEC = pl.BlockSpec(memory_space=HBM)


def run(kernel, arrays, out_shape, head=(), scratch=(), space=VMEM, **more):
    arrays = [pltpu.with_memory_space_constraint(x, space) for x in arrays]
    return pl.pallas_call(
        kernel,
        in_specs=[SMEM_SPEC] * len(head) + [pl.BlockSpec(memory_space=space)] * len(arrays),
        out_shape=out_shape,
        scratch_shapes=list(scratch),
        compiler_params=pltpu.CompilerParams(vmem_limit_bytes=24 * 2**20),
        **({"out_specs": jax.tree.map(lambda _: VMEM_SPEC, out_shape)} | more),
    )(*head, *arrays)


def sweep(
    onsite, broadening, hamiltonian, coupling, coupling_mask, prior_sigma,
    kernel_weights, kernel_offsets,
):
    layer_count = lax.axis_size("layer")
    group_count = lax.axis_size("energy")
    per_device = prior_sigma.shape[1]
    n = prior_sigma.shape[-1]
    span = 2 * per_device
    assert per_device == layer_count and layer_count & (layer_count - 1) == 0
    assert group_count % 4 == 0 and span > REACH
    ks = range(1, layer_count)

    everyone = [(l, g) for l in range(layer_count) for g in range(group_count)]

    def move(x, target, wanted=lambda l, g: True):
        pairs = []
        for l, g in everyone:
            tl, tg = target(l, g)
            if wanted(l, g) and 0 <= tg < group_count:
                pairs.append((l * group_count + g, tl * group_count + tg))
        return lax.ppermute(x, AXES, pairs)

    def to_layer(x, k):
        return move(x, lambda l, g: (l ^ k, g))

    def swapped(x):
        return move(x, lambda l, g: (l, g ^ 1))

    block = VMEM((2, n, n), F32)
    inputs = [coupling, coupling_mask, hamiltonian, onsite, broadening, prior_sigma]
    masked, quarter, *bases = run(
        prep_kernel, inputs, [block, VMEM((n // 2, n), F32)] + [block] * layer_count,
        scratch=[VMEM(x.shape, x.dtype) for x in inputs]
        + [pltpu.SemaphoreType.DMA((len(inputs),))],
        space=HBM,
    )
    quarters = [to_layer(quarter, k) for k in ks]
    moved = [
        [move(bases[k], lambda l, g: (l ^ k, g), lambda l, g: g % 2 == c) for k in ks]
        for c in range(2)
    ]
    weights = run(
        weight_kernel, [], VMEM((8 * -(-span // 8), 128), F32),
        [kernel_weights, kernel_offsets],
    )
    for _ in range(layer_count - 1):
        weights = run(tick_kernel, [weights], VMEM(weights.shape, F32))
    near = run(stack_kernel, quarters, VMEM((len(ks), n // 2, n), F32))
    far = move(near, lambda l, g: (l, g ^ 2))
    same = run(join_kernel, [near, far], VMEM((len(ks), n, n), F32))
    other = swapped(same)
    greens = run(
        functools.partial(solve_kernel, layer_count),
        [bases[0], *moved[0], *moved[1], masked, same, other], [block] * layer_count, scratch=[block] * 3,
    )

    mine = [greens[0]] + [to_layer(greens[k], k) for k in ks]

    def reached(l, g, k, step):
        spot = per_device * (g % 2) + (l ^ k)
        return (span - spot if step > 0 else spot + 1) <= REACH

    inner, outer = [], []
    for k in range(layer_count):
        def beyond(sign, k=k):
            step = lambda g: sign * (4 * (g % 2) - 2)
            return move(
                mine[k], lambda l, g: (l, g + step(g)),
                lambda l, g: reached(l, g, k, step(g)),
            )

        inner.append(beyond(1))
        outer.append(beyond(-1))
    final = layer_count - 1
    crossed = swapped(inner[final])
    kinds = {MINE: mine, INNER: inner, OUTER: outer, CROSSED: {final: crossed}}
    sums = VMEM((per_device, 2, n, n), F32)

    def slots_of(entries):
        return tuple(kind * layer_count + k for kind, k in entries)

    def mixed(accs, both, single=()):
        kernel = functools.partial(
            mix_kernel, slots_of(both), slots_of(single), accs is not None
        )
        blocks = [kinds[kind][k] for kind, k in (*both, *single)]
        return run(kernel, [*(accs or ()), *blocks], [sums, sums], [weights])

    every = range(layer_count)
    early = range(final - 1)
    sides = mixed(
        None, [(MINE, k) for k in every] + [(INNER, k) for k in early],
        [(OUTER, k) for k in early],
    )
    own, partner = mixed(sides, [(INNER, final - 1)], [(OUTER, final - 1)])
    given = swapped(partner)
    ending = [(INNER, final), (OUTER, final), (CROSSED, final)]
    shape = (1, per_device, 2, n, n)
    return run(
        functools.partial(last_kernel, slots_of(ending)),
        [own, given] + [kinds[kind][k] for kind, k in ending],
        jax.ShapeDtypeStruct(shape, F32), [weights],
        [VMEM(shape, F32), pltpu.SemaphoreType.DMA((2, 2))], out_specs=HBM_SPEC,
    )


def solution(mesh):
    placed = (
        P("layer", None),
        P("layer", None),
        P("layer", None, None, None),
        P("layer", None, None, None),
        P("layer", None, None),
        P("layer", "energy", None, None, None),
        P(),
        P(),
    )
    return jax.shard_map(
        sweep,
        mesh=mesh,
        in_specs=placed,
        out_specs=P("layer", "energy", None, None, None),
        check_vma=False,
    )
```

```python
import functools

import jax
import jax.numpy as jnp
from jax import lax
from jax.experimental import pallas as pl
from jax.experimental.pallas import tpu as pltpu
from jax.sharding import PartitionSpec as P


NS_ITERS = 3
REACH = 7

AXES = ("layer", "energy")
F32 = jnp.float32
BF16 = jnp.bfloat16
HBM = pltpu.HBM
VMEM = pltpu.VMEM


def split(x):
    high = x.astype(BF16)
    low = (x - high.astype(F32)).astype(BF16)
    return high, low


def dot(a, b, transposed):
    dims = (((1,), (1 if transposed else 0,)), ((), ()))
    return lax.dot_general(a, b, dims, preferred_element_type=F32)


def dot3(a, b, transposed=False):
    left = jnp.concatenate([a[0], a[0], a[1]], axis=1)
    right = jnp.concatenate([b[0], b[1], b[0]], axis=1 if transposed else 0)
    return dot(left, right, transposed)


def product(a, b):
    rr = dot3(a[0], b[0])
    ii = dot3(a[1], b[1])
    return rr - ii, dot3(a[2], b[2]) - rr - ii


def product_adjoint(a, c):
    rr = dot3(a[0], c[0], True)
    ii = dot3(a[1], c[1], True)
    return rr + ii, dot3(a[2], c[3], True) - rr + ii


def split_pair(pair):
    return split(pair[0]), split(pair[1]), split(pair[0] + pair[1]), split(pair[0] - pair[1])


def eye_mask(n):
    return lax.broadcasted_iota(jnp.int32, (n, n), 0) == lax.broadcasted_iota(
        jnp.int32, (n, n), 1
    )


def inverse_of(real, imag):
    n = real.shape[0]
    eye = eye_mask(n)
    zero = jnp.zeros_like(real)
    diag_real = jnp.where(eye, real, zero)
    diag_imag = jnp.where(eye, imag, zero)

    def reciprocal(axis):
        dr = jnp.sum(diag_real, axis=axis, keepdims=True)
        di = jnp.sum(diag_imag, axis=axis, keepdims=True)
        modulus = dr * dr + di * di
        return dr / modulus, -di / modulus

    row_r, row_i = reciprocal(0)
    col_r, col_i = reciprocal(1)
    e_r = jnp.where(eye, zero, real * -row_r + imag * row_i)
    e_i = jnp.where(eye, zero, real * -row_i - imag * row_r)
    unit = jnp.where(eye, 1.0, 0.0).astype(F32)
    f_r, f_i = unit + e_r, e_i
    for _ in range(NS_ITERS - 1):
        es = split_pair((e_r, e_i))
        e_r, e_i = product(es, es)
        es = split_pair((e_r, e_i))
        g_r, g_i = product(split_pair((f_r, f_i)), es)
        f_r, f_i = f_r + g_r, f_i + g_i
    return col_r * f_r - col_i * f_i, col_r * f_i + col_i * f_r


def turn(layer_count):
    return layer_count // 2


def prep_kernel(
    coup_hbm, mask_hbm, ham_hbm, onsite_hbm, broad_hbm, prior_hbm, masked_ref, quarter_ref, *refs
):
    base_refs = refs[:-7]
    coup_ref, mask_ref, ham_ref, onsite_ref, broad_ref, prior_ref, sems = refs[-7:]
    sources = (coup_hbm, mask_hbm, ham_hbm, onsite_hbm, broad_hbm, prior_hbm)
    targets = (coup_ref, mask_ref, ham_ref, onsite_ref, broad_ref, prior_ref)
    copies = [
        pltpu.make_async_copy(source, target, sems.at[i])
        for i, (source, target) in enumerate(zip(sources, targets))
    ]
    for copy in copies:
        copy.start()
    per_device = prior_ref.shape[1]
    layer = lax.axis_index("layer")
    group = lax.axis_index("energy")
    plane, half = group % 2, (group // 2) % 2
    rows = quarter_ref.shape[0]
    for copy in copies[:2]:
        copy.wait()
    mask = mask_ref[0].astype(F32)
    c_r, c_i = coup_ref[0, 0] * mask, coup_ref[0, 1] * mask
    masked_ref[0], masked_ref[1] = c_r, c_i
    here = pl.ds(pl.multiple_of(half * rows, rows), rows)
    quarter_ref[...] = masked_ref[plane, here, :]
    cs = split_pair((c_r, c_i))
    q_r, q_i = product_adjoint(cs, cs)
    for copy in copies[2:5]:
        copy.wait()
    first = group * per_device
    grid_size = per_device * lax.axis_size("energy")
    n = ham_ref.shape[-1]
    h_r, h_i = ham_ref[0, 0], ham_ref[0, 1]
    eye = eye_mask(n)
    own = jnp.where(layer == 0, 0.5, 0.0).astype(F32)
    fixed_r = -0.5 * (h_r + h_r.T) - own * q_i + jnp.where(eye, -onsite_ref[...], 0.0)
    fixed_i = -0.5 * (h_i - h_i.T) + own * q_r + jnp.where(eye, broad_ref[...], 0.0)
    copies[5].wait()
    for k, base_ref in enumerate(base_refs):
        mine = jnp.bitwise_xor(layer, k ^ turn(len(base_refs)))
        level = -1.0 + 2.0 * ((first + mine).astype(F32) + 0.5) / grid_size
        base_ref[0] = fixed_r - prior_ref[0, mine, 0] + jnp.where(eye, level, 0.0)
        base_ref[1] = fixed_i - prior_ref[0, mine, 1]


def stack_kernel(*refs):
    out_ref = refs[-1]
    for k, ref in enumerate(refs[:-1]):
        out_ref[k] = ref[...]


def join_kernel(near_ref, far_ref, out_ref):
    half = (lax.axis_index("energy") // 2) % 2
    rows = near_ref.shape[1]
    for side, ref in ((half, near_ref), (1 - half, far_ref)):
        out_ref[:, pl.ds(pl.multiple_of(side * rows, rows), rows), :] = ref[...]


def solve_kernel(layer_count, *refs):
    refs = list(refs)
    take = lambda count: [refs.pop(0) for _ in range(count)]
    (own_base,) = take(1)
    base_refs = [take(layer_count - 1) for _ in range(2)]
    masked_ref, same_ref, other_ref = take(3)
    out_refs = take(layer_count)
    system, coup, green = refs
    layer = lax.axis_index("layer")
    core = lax.axis_index("energy") % 2

    def step(l, carry):
        source = jnp.bitwise_xor(layer, l)

        @pl.when(source == 0)
        def _():
            system[...] = own_base[...]
            coup[...] = masked_ref[...]

        for k in range(1, layer_count):
            @pl.when(source == k)
            def _(k=k):
                coup[core] = same_ref[k - 1]
                coup[1 - core] = other_ref[k - 1]

            for c in range(2):
                @pl.when((source == k) & (core == c))
                def _(k=k, c=c):
                    system[...] = base_refs[c][k - 1][...]

        @pl.when(l > 0)
        def _():
            cs = split_pair((coup[0], coup[1]))
            moved = product(cs, split_pair((green[0], green[1])))
            contact_r, contact_i = product_adjoint(split_pair(moved), cs)
            system[0] -= contact_r
            system[1] -= contact_i

        g_r, g_i = inverse_of(system[0], system[1])
        green[0], green[1] = g_r, g_i
        for k in range(layer_count):
            @pl.when(source == k)
            def _(k=k):
                out_refs[k][0], out_refs[k][1] = g_r, g_i
        return carry

    lax.fori_loop(0, layer_count, step, 0, unroll=True)


STEP_ROWS = 16


MINE, INNER, OUTER, CROSSED = range(4)


def weight_kernel(value_ref, offset_ref, out_ref):
    layer = lax.axis_index("layer")
    core = lax.axis_index("energy") % 2
    layer_count = lax.axis_size("layer")
    per_device = layer_count
    shape = out_ref.shape
    row = lax.broadcasted_iota(jnp.int32, shape, 0)
    lane = lax.broadcasted_iota(jnp.int32, shape, 1)
    kind = lane // layer_count
    away = 2 * core - 1
    shift = jnp.where(kind == INNER, -away, jnp.where(kind == MINE, 0, away))
    far_core = jnp.where(kind == CROSSED, 1 - core, core)
    source = jnp.bitwise_xor((lane % layer_count) ^ turn(layer_count), layer)
    target = jnp.where(row < per_device, per_device * core, -per_device * core) + row
    gap = 2 * per_device * shift + per_device * far_core + source - target
    total = jnp.zeros(shape, F32)
    for tap in range(value_ref.shape[0]):
        total += jnp.where(gap == offset_ref[tap], value_ref[tap], 0.0)
    out_ref[...] = total


STEP_ROWS = 8


def add_blocks(total, weight_ref, slots, refs, part, here, first_row):
    total = list(total)
    for slot, ref in zip(slots, refs):
        x = ref[part, here, :]
        for f in range(len(total)):
            term = weight_ref[first_row + f, slot] * x
            total[f] = term if total[f] is None else total[f] + term
    return total


def tick_kernel(in_ref, out_ref):
    out_ref[...] = in_ref[...]


def mix_kernel(both, single, has_acc, weight_ref, *refs):
    refs = list(refs)
    own_ref, partner_ref = refs[-2:]
    accs = refs[:2] if has_acc else None
    blocks = refs[2 if has_acc else 0 : -2]
    outputs, parts, rows, _ = own_ref.shape
    for part in range(parts):
        def body(i, carry, part=part):
            here = pl.ds(pl.multiple_of(i * STEP_ROWS, STEP_ROWS), STEP_ROWS)
            for side, (target, slots) in enumerate(
                ((own_ref, both + single), (partner_ref, both))
            ):
                total = [accs[side][f, part, here, :] if has_acc else None for f in range(outputs)]
                total = add_blocks(
                    total, weight_ref, slots, blocks[: len(slots)], part, here, side * outputs
                )
                for f in range(outputs):
                    target[f, part, here, :] = total[f]
            return carry

        lax.fori_loop(0, rows // STEP_ROWS, body, 0, unroll=2)


def last_kernel(slots, weight_ref, own_ref, partner_ref, *refs):
    blocks, out_ref, buffer, sems = refs[:-3], refs[-3], refs[-2], refs[-1]
    outputs, parts, rows, _ = own_ref.shape
    pieces = sems.shape[1]
    size = rows // pieces
    copies = []
    for part in range(parts):
        for piece in range(pieces):
            def body(i, carry, part=part, base=piece * size):
                here = pl.ds(pl.multiple_of(base + i * STEP_ROWS, STEP_ROWS), STEP_ROWS)
                total = [
                    own_ref[f, part, here, :] + partner_ref[f, part, here, :]
                    for f in range(outputs)
                ]
                total = add_blocks(total, weight_ref, slots, blocks, part, here, 0)
                for f in range(outputs):
                    buffer[0, f, part, here, :] = total[f]
                return carry

            lax.fori_loop(0, size // STEP_ROWS, body, 0, unroll=4)
            here = (slice(None), slice(None), part, pl.ds(piece * size, size))
            copy = pltpu.make_async_copy(buffer.at[here], out_ref.at[here], sems.at[part, piece])
            copy.start()
            copies.append(copy)
    for copy in copies:
        copy.wait()


SMEM_SPEC = pl.BlockSpec(memory_space=pltpu.SMEM)
VMEM_SPEC = pl.BlockSpec(memory_space=VMEM)
HBM_SPEC = pl.BlockSpec(memory_space=HBM)


def run(kernel, arrays, out_shape, head=(), scratch=(), space=VMEM, **more):
    arrays = [pltpu.with_memory_space_constraint(x, space) for x in arrays]
    return pl.pallas_call(
        kernel,
        in_specs=[SMEM_SPEC] * len(head) + [pl.BlockSpec(memory_space=space)] * len(arrays),
        out_shape=out_shape,
        scratch_shapes=list(scratch),
        compiler_params=pltpu.CompilerParams(vmem_limit_bytes=24 * 2**20),
        **({"out_specs": jax.tree.map(lambda _: VMEM_SPEC, out_shape)} | more),
    )(*head, *arrays)


def sweep(
    onsite, broadening, hamiltonian, coupling, coupling_mask, prior_sigma,
    kernel_weights, kernel_offsets,
):
    layer_count = lax.axis_size("layer")
    group_count = lax.axis_size("energy")
    per_device = prior_sigma.shape[1]
    n = prior_sigma.shape[-1]
    span = 2 * per_device
    assert per_device == layer_count and layer_count & (layer_count - 1) == 0
    assert group_count % 4 == 0 and span > REACH
    ks = range(1, layer_count)

    everyone = [(l, g) for l in range(layer_count) for g in range(group_count)]

    def move(x, target, wanted=lambda l, g: True):
        pairs = []
        for l, g in everyone:
            tl, tg = target(l, g)
            if wanted(l, g) and 0 <= tg < group_count:
                pairs.append((l * group_count + g, tl * group_count + tg))
        return lax.ppermute(x, AXES, pairs)

    def to_layer(x, k):
        return move(x, lambda l, g: (l ^ k, g))

    def swapped(x):
        return move(x, lambda l, g: (l, g ^ 1))

    block = VMEM((2, n, n), F32)
    inputs = [coupling, coupling_mask, hamiltonian, onsite, broadening, prior_sigma]
    masked, quarter, *bases = run(
        prep_kernel, inputs, [block, VMEM((n // 2, n), F32)] + [block] * layer_count,
        scratch=[VMEM(x.shape, x.dtype) for x in inputs]
        + [pltpu.SemaphoreType.DMA((len(inputs),))],
        space=HBM,
    )
    quarters = [to_layer(quarter, k) for k in ks]
    moved = [
        [move(bases[k], lambda l, g: (l ^ k, g), lambda l, g: g % 2 == c) for k in ks]
        for c in range(2)
    ]
    weights = run(
        weight_kernel, [], VMEM((8 * -(-span // 8), 128), F32),
        [kernel_weights, kernel_offsets],
    )
    for _ in range(layer_count - 1):
        weights = run(tick_kernel, [weights], VMEM(weights.shape, F32))
    near = run(stack_kernel, quarters, VMEM((len(ks), n // 2, n), F32))
    far = move(near, lambda l, g: (l, g ^ 2))
    same = run(join_kernel, [near, far], VMEM((len(ks), n, n), F32))
    other = swapped(same)
    greens = run(
        functools.partial(solve_kernel, layer_count),
        [bases[0], *moved[0], *moved[1], masked, same, other], [block] * layer_count, scratch=[block] * 3,
    )

    mine = [greens[0]] + [to_layer(greens[k], k) for k in ks]

    def reached(l, g, k, step):
        spot = per_device * (g % 2) + (l ^ k ^ turn(layer_count))
        return (span - spot if step > 0 else spot + 1) <= REACH

    inner, outer = [], []
    for k in range(layer_count):
        def beyond(sign, k=k):
            step = lambda g: sign * (4 * (g % 2) - 2)
            return move(
                mine[k], lambda l, g: (l, g + step(g)),
                lambda l, g: reached(l, g, k, step(g)),
            )

        inner.append(beyond(1))
        outer.append(beyond(-1))
    final = layer_count - 1
    crossed = swapped(inner[final])
    kinds = {MINE: mine, INNER: inner, OUTER: outer, CROSSED: {final: crossed}}
    sums = VMEM((per_device, 2, n, n), F32)

    def slots_of(entries):
        return tuple(kind * layer_count + k for kind, k in entries)

    def mixed(accs, both, single=()):
        kernel = functools.partial(
            mix_kernel, slots_of(both), slots_of(single), accs is not None
        )
        blocks = [kinds[kind][k] for kind, k in (*both, *single)]
        return run(kernel, [*(accs or ()), *blocks], [sums, sums], [weights])

    every = range(layer_count)
    early = range(final - 1)
    sides = mixed(
        None, [(MINE, k) for k in every] + [(INNER, k) for k in early],
        [(OUTER, k) for k in early],
    )
    own, partner = mixed(sides, [(INNER, final - 1)], [(OUTER, final - 1)])
    given = swapped(partner)
    ending = [(INNER, final), (OUTER, final), (CROSSED, final)]
    shape = (1, per_device, 2, n, n)
    return run(
        functools.partial(last_kernel, slots_of(ending)),
        [own, given] + [kinds[kind][k] for kind, k in ending],
        jax.ShapeDtypeStruct(shape, F32), [weights],
        [VMEM(shape, F32), pltpu.SemaphoreType.DMA((2, 4))], out_specs=HBM_SPEC,
    )


def solution(mesh):
    placed = (
        P("layer", None),
        P("layer", None),
        P("layer", None, None, None),
        P("layer", None, None, None),
        P("layer", None, None),
        P("layer", "energy", None, None, None),
        P(),
        P(),
    )
    return jax.shard_map(
        sweep,
        mesh=mesh,
        in_specs=placed,
        out_specs=P("layer", "energy", None, None, None),
        check_vma=False,
    )
```
